256 devices in a mesh: rows: 32 (over y, x, core), hub: 8 (over z).
Axes of the slice: x: 4, y: 4, z: 8, core: 2. Of those that a mesh axis runs over, the one named last changes fastest.
Arguments:
- tail_blocks: float32 [18432, 128, 128], P(('rows', 'hub')), may hold values from -0.21875 to 0.21875
- tail_row: int32 [18432], P(('rows', 'hub')), may hold values from 0 to 15
- tail_owner: int32 [18432, 1], P(('rows', 'hub')), may hold values from 0 to 31; in each aligned block of 72 rows (0 to 71, 72 to 143, ...) at most 6 rows name the same one
- tail_slot: int32 [18432], P(('rows', 'hub')), may hold values from 0 to 63
- hub_blocks: float32 [6144, 128, 128], P(('rows', 'hub')), may hold values from -0.21875 to 0.21875
- hub_row: int32 [6144], P(('rows', 'hub')), may hold values from 0 to 15
- hub_col: int32 [6144], P(('rows', 'hub')), may hold values from 0 to 255
- x_tail: float32 [16384, 128], P(('rows', 'hub')), may hold values from 0 to 0.5
- cost_tail: float32 [16384, 128], P(('rows', 'hub')), may hold values from -6 to 6
- upper_tail: float32 [16384, 128], P(('rows', 'hub')), may hold values from 0.5 to 2
- x_hub: float32 [256, 128], P('hub'), may hold values from 0 to 0.5
- cost_hub: float32 [256, 128], P('hub'), may hold values from -6 to 6
- upper_hub: float32 [256, 128], P('hub'), may hold values from 0.5 to 2
- duals: float32 [4096, 128], P(('rows', 'hub')), may hold values from 0 to 1
- demand: float32 [4096, 128], P(('rows', 'hub')), may hold values from -6 to 6
Outputs:
- x_tail_out: float32 [16384, 128], P(('rows', 'hub'))
- x_hub_out: float32 [256, 128], P('hub')
- duals_out: float32 [4096, 128], P(('rows', 'hub'))
The draws below stay inside these ranges and needn't reach their ends.
Inputs may be any that keep to these rules, and one draw needn't show every extreme that they name: `tail_owner`: among the blocks of one device no owner is named more than 6 times; on some device one owner is named exactly 6 times.
All inputs are finite; a program needn't handle non-finite values.
Results may differ from the reference program's by a relative error of at most 0.0001.
Values sent between devices are 32-bit elements; how exact they have to be, the bound alone decides.
A program may use at most 64 MiB of HBM per device.

```python
import math
import jax
import jax.numpy as jnp
import numpy as np
from jax import lax

BW = 128
NB_DEV = 72
HNB_DEV = 24
CB_DEV = 64
RB_DEV = 16
ITERS = 3
CAP = 6
TAILB = 16384
HUBB = 256
ROWB = 4096
TAILN = 18432
HUBN = 6144
N_ROWS = 32
N_HUB = 8


def place_ends(entries, rng, low, largest):
    extent = entries.shape
    index_at = [jax.random.randint(jax.random.fold_in(rng, axis), (), 0, extent[axis]) for axis in range(len(extent))]
    entries = entries.at[tuple(index_at)].set(low)
    longest = extent.index(max(extent))
    index_at[longest] = (index_at[longest] + 1) % extent[longest]
    return entries.at[tuple(index_at)].set(largest)


def block_levels(stream_key, dims, split, smallest, high):
    gain, own = 1.0, jax.random.fold_in(stream_key, 6)
    for axis_at, blocks in split:
        heights = jnp.exp(jax.random.uniform(jax.random.fold_in(own, axis_at), (blocks,), jnp.float32, smallest / len(split), high / len(split)))
        gain = gain * jnp.repeat(heights, dims[axis_at] // blocks).reshape([-1 if axis == axis_at else 1 for axis in range(len(dims))])
    return gain


def rank_bounds(number_of, skew):
    portions = [(1 << 20) // math.isqrt(standing ** skew) + 1 for standing in range(1, number_of + 1)]
    deviation = 1 + sum(portions) // (1 << 30)
    return np.cumsum(np.array([max(1, weight // deviation) for weight in portions]))


def skewed_ids(rng, extent, count, lean):
    table = rank_bounds(count, lean)
    ticket = jax.random.randint(jax.random.fold_in(rng, 1), extent, 0, int(table[count - 1]))
    rank = jnp.searchsorted(jnp.asarray(table, jnp.int32), ticket, side="right")
    return jax.random.permutation(jax.random.fold_in(rng, 2), count)[rank].astype(jnp.int32)


def deal_out(own_key, own, number, rows, amount, top, most, lean):
    order = jax.random.permutation(own_key, amount)
    heavy_load, ordinary = portions_of(amount, rows * top, most, lean, True), portions_of(amount, rows * top, most, lean, False)
    places = jnp.arange(amount)

    def named(sizes, turn):
        used = int((sizes > 0).sum())
        fixed = max(1, used // 4)
        shifted = fixed + (places - fixed + turn * (used - fixed)) % max(1, amount - fixed)
        return jnp.zeros((amount,), jnp.int32).at[order[jnp.where(places < fixed, places, shifted)]].set(jnp.asarray(sizes, jnp.int32))

    sizes = jnp.where(number % 4 == 0, named(heavy_load, number // 4), named(ordinary, number - number // 4 - 1))
    mixed = jax.random.permutation(jax.random.fold_in(own, 3), amount)
    giver, sink = mixed[0:amount // 2 * 2:2], mixed[1:amount // 2 * 2:2]
    margin = jnp.minimum(sizes[giver] - 1, most - sizes[sink]) // 2
    margin = jnp.where((giver == order[0]) | (sink == order[0]) | (sizes[sink] == 0), 0, jnp.maximum(margin, 0))
    shifted = jax.random.randint(jax.random.fold_in(own, 4), (amount // 2,), 0, 1 << 20) % (margin + 1)
    sizes = sizes.at[giver].add(-shifted).at[sink].add(shifted)
    items = jnp.searchsorted(jnp.cumsum(sizes), jnp.arange(rows * top), side="right").astype(jnp.int32)
    table = items.reshape(top, rows).T
    table = table[jax.random.permutation(jax.random.fold_in(own, 1), rows)]
    turn = jax.random.randint(jax.random.fold_in(own, 2), (rows, 1), 0, top)
    return jnp.take_along_axis(table, (jnp.arange(top)[None, :] + turn) % top, axis=1)


def portions_of(amount, total, bound, slope, full):
    weights = [(1 << 20) // math.isqrt(standing ** slope) + 1 for standing in range(1, amount + 1)]
    largest = bound if full else min(bound, max(-(-total // amount), total * weights[0] // sum(weights)))
    least = 1 if total - largest >= amount - 1 else 0
    given, rest = [largest] + [least] * (amount - 1), total - largest - least * (amount - 1)
    while rest > 0:
        free = [i for i in range(1, amount) if given[i] < largest] or [i for i in range(1, amount) if given[i] < bound]
        mass, budget = sum([weights[i] for i in free]), rest
        for i in free:
            extra = min(bound - given[i], max(1, budget * weights[i] // mass), rest)
            given[i] = given[i] + extra
            rest = rest - extra
    return np.array(given)


def scatter_about(stream_key, shape, spread, bound, split=(), kind=jnp.bfloat16):
    array = spread * jax.random.normal(stream_key, shape, jnp.float32)
    if split:
        array = array * block_levels(stream_key, shape, split, -0.22, 0.18)
    return jnp.clip(array, -bound, bound).astype(kind)


def setup_inputs(seed: int = 0) -> dict:
    arg_keys = jax.random.split(jax.random.key(seed), 16)
    tail_blocks = scatter_about(arg_keys[0], (TAILN, BW, BW), (BW * (NB_DEV + HNB_DEV) // RB_DEV) ** -0.5, 0.21875, ((0, 256),), jnp.float32)
    tail_row = place_ends(jax.random.randint(arg_keys[1], (TAILN,), 0, RB_DEV), jax.random.fold_in(arg_keys[1], 1), 0, RB_DEV - 1).astype(jnp.int32)
    tail_owner_keys = jax.random.split(jax.random.fold_in(arg_keys[2], 1), TAILN // NB_DEV)
    tail_owner_turns = jax.random.permutation(jax.random.fold_in(arg_keys[2], 3), TAILN // NB_DEV)
    tail_owner = jax.vmap(lambda own, number: deal_out(jax.random.fold_in(arg_keys[2], 2), own, number, NB_DEV, N_ROWS, 1, CAP, 2))(tail_owner_keys, tail_owner_turns).reshape((TAILN, 1))
    tail_slot = place_ends(jax.random.randint(arg_keys[3], (TAILN,), 0, CB_DEV), jax.random.fold_in(arg_keys[3], 1), 0, CB_DEV - 1).astype(jnp.int32)
    hub_blocks = scatter_about(arg_keys[4], (HUBN, BW, BW), (BW * (NB_DEV + HNB_DEV) // RB_DEV) ** -0.5, 0.21875, ((0, 256),), jnp.float32)
    hub_row = place_ends(jax.random.randint(arg_keys[5], (HUBN,), 0, RB_DEV), jax.random.fold_in(arg_keys[5], 1), 0, RB_DEV - 1).astype(jnp.int32)
    hub_col = place_ends(skewed_ids(arg_keys[6], (HUBN,), HUBB, 2), jax.random.fold_in(arg_keys[6], 3), 0, HUBB - 1).astype(jnp.int32)
    x_tail = jnp.clip(0.5 * jax.random.uniform(arg_keys[7], (TAILB, BW), jnp.float32) ** block_levels(arg_keys[7], (TAILB, BW), ((0, 256),), -0.2, 0.2), 0.0, 0.5)
    cost_tail = scatter_about(arg_keys[8], (TAILB, BW), 1.0, 6.0, ((0, 256),), jnp.float32)
    upper_tail = jnp.clip(jnp.exp(math.log(2.0) - 1.3862944 * jax.random.uniform(arg_keys[9], (TAILB, BW), jnp.float32) ** block_levels(arg_keys[9], (TAILB, BW), ((0, 256),), -0.2, 0.2)), 0.5, 2.0)
    x_hub = jnp.clip(0.5 * jax.random.uniform(arg_keys[10], (HUBB, BW), jnp.float32) ** block_levels(arg_keys[10], (HUBB, BW), ((0, 8),), -0.2, 0.2), 0.0, 0.5)
    cost_hub = scatter_about(arg_keys[11], (HUBB, BW), 1.0, 6.0, ((0, 8),), jnp.float32)
    upper_hub = jnp.clip(jnp.exp(math.log(2.0) - 1.3862944 * jax.random.uniform(arg_keys[12], (HUBB, BW), jnp.float32) ** block_levels(arg_keys[12], (HUBB, BW), ((0, 8),), -0.2, 0.2)), 0.5, 2.0)
    duals = jnp.clip(1.0 * jax.random.uniform(arg_keys[13], (ROWB, BW), jnp.float32) ** block_levels(arg_keys[13], (ROWB, BW), ((0, 256),), -0.2, 0.2), 0.0, 1.0)
    demand = scatter_about(arg_keys[14], (ROWB, BW), 1.0, 6.0, ((0, 256),), jnp.float32)
    return dict(tail_blocks=tail_blocks, tail_row=tail_row, tail_owner=tail_owner, tail_slot=tail_slot, hub_blocks=hub_blocks, hub_row=hub_row, hub_col=hub_col, x_tail=x_tail, cost_tail=cost_tail, upper_tail=upper_tail, x_hub=x_hub, cost_hub=cost_hub, upper_hub=upper_hub, duals=duals, demand=demand)


primal_step = 0.25
dual_step = 0.25


def forward_product(blocks, row_index, col_index, vector, row_count):
    picked = vector[col_index]
    product = jnp.einsum("bij,bj->bi", blocks, picked, precision=lax.Precision.HIGHEST)
    return jax.ops.segment_sum(product, row_index, num_segments=row_count)


def adjoint_product(blocks, row_index, col_index, weights, col_count):
    picked = weights[row_index]
    product = jnp.einsum("bij,bi->bj", blocks, picked, precision=lax.Precision.HIGHEST)
    return jax.ops.segment_sum(product, col_index, num_segments=col_count)


def reference(tail_blocks, tail_row, tail_owner, tail_slot, hub_blocks, hub_row, hub_col, x_tail, cost_tail, upper_tail, x_hub, cost_hub, upper_hub, duals, demand):
    tail_count = tail_blocks.shape[0]
    hub_count = hub_blocks.shape[0]
    row_count = duals.shape[0]
    device_of = (jnp.arange(tail_count, dtype=jnp.int32) // NB_DEV).astype(jnp.int32)
    tail_rows = (device_of * RB_DEV + tail_row).astype(jnp.int32)
    tail_cols = ((tail_owner[:, 0] * N_HUB + device_of % N_HUB) * CB_DEV + tail_slot).astype(jnp.int32)
    hub_device = (jnp.arange(hub_count, dtype=jnp.int32) // HNB_DEV).astype(jnp.int32)
    hub_rows = (hub_device * RB_DEV + hub_row).astype(jnp.int32)
    hub_cols = hub_col.astype(jnp.int32)
    for iteration in range(ITERS):
        image_tail = adjoint_product(tail_blocks, tail_rows, tail_cols, duals, x_tail.shape[0])
        image_hub = adjoint_product(hub_blocks, hub_rows, hub_cols, duals, x_hub.shape[0])
        tail_next = jnp.minimum(jnp.maximum(x_tail - primal_step * (cost_tail - image_tail), 0.0), upper_tail)
        hub_next = jnp.minimum(jnp.maximum(x_hub - primal_step * (cost_hub - image_hub), 0.0), upper_hub)
        tail_extra = 2.0 * tail_next - x_tail
        hub_extra = 2.0 * hub_next - x_hub
        primal_image = forward_product(tail_blocks, tail_rows, tail_cols, tail_extra, row_count)
        primal_image = primal_image + forward_product(hub_blocks, hub_rows, hub_cols, hub_extra, row_count)
        duals = jnp.maximum(duals + dual_step * (demand - primal_image), 0.0)
        x_tail = tail_next
        x_hub = hub_next
    return (x_tail, x_hub, duals)
```

```python
import jax
import jax.numpy as jnp
from jax import lax
from jax.experimental import pallas as pl
from jax.experimental.pallas import tpu as pltpu
from jax.sharding import PartitionSpec as P

ITERS = 3
PRIMAL = 0.25
DUAL = 0.25
MESH = pl.DeviceIdType.MESH
F32 = jnp.float32
BF16 = jnp.bfloat16

NT = 72
NH = 24
NR = 16
NC = 64
CAP = 6
BW = 128
ROWS = 32
HUBS = 8
TP = 80
HP = 32
PL = 8 * ROWS


def hops(d):
    return min(d, 4 - d)


OFFSETS = sorted(
    [(dy, dx, dc) for dy in range(4) for dx in range(4) for dc in range(2) if dy or dx or dc],
    key=lambda o: (-(hops(o[0]) + hops(o[1])), -o[2], o[0], o[1]),
)
HUB_OFFSETS = [4, 3, 5, 2, 6, 1, 7]


def iota(shape, dim):
    return lax.broadcasted_iota(jnp.int32, shape, dim)


def split3(a):
    hi = a.astype(BF16)
    rest = a - hi.astype(F32)
    mid = rest.astype(BF16)
    lo = (rest - mid.astype(F32)).astype(BF16)
    return hi, mid, lo


def mm(a, b):
    return jnp.dot(a, b, preferred_element_type=F32)


def kernel(
    tail_hbm, tail_row, owner_ref, tail_slot, hub_hbm, hub_row, hub_col,
    x_tail, cost_tail, upper_tail, x_hub, cost_hub, upper_hub, duals, demand,
    xt_out, xh_out, d_out,
    tb, hb, dbc,
    hub_out, hub_in, z_out, z_in, ag_out, ag_in,
    tail_out, tail_in, ans_out, ans_in,
    slot_out, slot_in, init_out, init_in, xf_out, xf_in,
    terms, hterms, picked, colbuf,
    s3, hp3, ct3, coll, st, rp, xh_state, d_state, dem_t,
    load_sem, s_sem, r_sem,
):
    me = lax.axis_index("rows")
    hub = lax.axis_index("hub")
    y, x, c = me // 8, lax.rem(me // 2, 4), lax.rem(me, 2)
    peers = [
        lax.rem(y + dy, 4) * 8 + lax.rem(x + dx, 4) * 2 + lax.rem(c + dc, 2) for dy, dx, dc in OFFSETS
    ]
    hub_peers = [lax.rem(hub + d, HUBS) for d in HUB_OFFSETS]

    def at8(i, n=8):
        return pl.ds(pl.multiple_of(i * 8, 8), n)

    loads = [pltpu.make_async_copy(hub_hbm, hb, load_sem.at[0])]
    loads[0].start()
    step = NT // 4
    for i in range(4):
        part = pl.ds(i * step, step)
        loads.append(pltpu.make_async_copy(tail_hbm.at[part], tb.at[part], load_sem.at[1 + i]))
        loads[-1].start()

    barrier = pltpu.get_barrier_semaphore()
    for p in peers:
        pl.semaphore_signal(barrier, inc=1, device_id={"rows": p}, device_id_type=MESH)
    for p in hub_peers:
        pl.semaphore_signal(barrier, inc=1, device_id={"hub": p}, device_id_type=MESH)

    def to_rows(src, dst, k):
        for p in peers:
            pltpu.make_async_remote_copy(
                src_ref=src(p), dst_ref=dst, send_sem=s_sem.at[k], recv_sem=r_sem.at[k],
                device_id={"rows": p}, device_id_type=MESH,
            ).start()

    def to_hubs(src, dst, k):
        for p in hub_peers:
            pltpu.make_async_remote_copy(
                src_ref=src, dst_ref=dst, send_sem=s_sem.at[k], recv_sem=r_sem.at[k],
                device_id={"hub": p}, device_id_type=MESH,
            ).start()

    def wait_bytes(ref, sem):
        pltpu.make_async_copy(ref, ref, sem).wait()

    for b in range(NT):
        colbuf[pl.ds(b, 1), :] = jnp.full((1, BW), tail_slot[b], jnp.int32).astype(F32)
    slot_col = jnp.where(iota((TP, BW), 0) < NT, colbuf[0:TP, :], 0.0)
    own = jnp.broadcast_to(owner_ref[...].astype(F32), (NT, BW))
    own_col = jnp.concatenate([own, jnp.full((BW - NT, BW), -1.0, F32)], axis=0)
    own_row = own_col.T
    sub, lane = iota((BW, BW), 0), iota((BW, BW), 1)
    before = jnp.where((own_col == own_row) & (lane < sub), 1.0, 0.0)
    within = jnp.sum(before, axis=1, keepdims=True)
    place = jnp.where(sub < NT, own_col * 8.0 + within, -1.0)
    place = place[0:TP, :]
    place3 = jnp.concatenate([place, place, place, jnp.full((16, BW), -1.0, F32)], axis=0)
    place_row = place3.T[0:1, :]
    s3[...] = jnp.where(iota((PL, 256), 0).astype(F32) == place_row, 1.0, 0.0).astype(BF16)
    st[...] = jnp.where(
        iota((TP, PL), 1).astype(F32) == jnp.concatenate([place, place], axis=1), 1.0, 0.0
    ).astype(BF16)
    zeros16 = jnp.zeros((16, BW), BF16)
    slot_b = slot_col.astype(BF16)
    zeros_tp = jnp.zeros((TP, BW), BF16)
    slot_out[...] = mm(s3[...], jnp.concatenate([slot_b, zeros_tp, zeros_tp, zeros16], axis=0))

    init_out[...] = jnp.zeros((8, BW), F32)
    init_out[0:1, :] = x_hub[pl.ds(me, 1), :]
    init_out[1:2, :] = cost_hub[pl.ds(me, 1), :]
    init_out[2:3, :] = upper_hub[pl.ds(me, 1), :]

    pl.semaphore_wait(barrier, len(OFFSETS) + len(HUB_OFFSETS))

    to_rows(lambda p: slot_out.at[at8(p, CAP), :], slot_in.at[at8(me, CAP), :], 15)
    to_hubs(init_out, init_in.at[at8(hub), :], 16)

    pos_row = jnp.full((1, BW), -1, jnp.int32)
    lane1 = iota((1, BW), 1)
    for k in range(NH):
        col = hub_col[k]
        pos = lax.rem(col, ROWS) * 8 + col // ROWS
        pos_row = jnp.where((lane1 % HP == k) & (lane1 < 3 * HP), pos, pos_row)
    hp3[...] = jnp.where(iota((PL, BW), 0) == pos_row, 1.0, 0.0).astype(BF16)

    for b in range(NT):
        colbuf[pl.ds(b, 1), :] = jnp.full((1, BW), tail_row[b], jnp.int32).astype(F32)
    for k in range(NH):
        colbuf[pl.ds(NT + k, 1), :] = jnp.full((1, BW), hub_row[k], jnp.int32).astype(F32)
    rp[...] = jnp.where(
        (colbuf[...] == lane.astype(F32)) & (sub < NT + NH), 1.0, 0.0
    ).astype(BF16)

    pad = jnp.zeros((BW - NR, BW), F32)
    dem_t[...] = jnp.concatenate([demand[...], pad], axis=0).T
    d_t = jnp.concatenate([duals[...], pad], axis=0).T
    d_state[...] = d_t
    for r in range(NR):
        dbc[r] = jnp.broadcast_to(d_t[:, r : r + 1], (BW, BW))

    terms[...] = jnp.zeros_like(terms)
    hterms[...] = jnp.zeros_like(hterms)
    xt_out[...] = x_tail[...]
    live = lax.rem(iota((PL, BW), 0), 8) < CAP

    loads[0].wait()

    def iteration(it, carry):
        def hub_adj(k, cc):
            hterms[pl.ds(k, 1), :] = jnp.sum(hb[k] * dbc[hub_row[k]], axis=0, keepdims=True)
            return cc

        lax.fori_loop(0, NH, hub_adj, 0, unroll=4)
        hi, mid, lo = split3(hterms[...])
        hub_out[it] = mm(hp3[...], jnp.concatenate([hi, mid, lo, jnp.zeros_like(hi)], axis=0))
        to_rows(lambda p: hub_out.at[it, at8(p), :], hub_in.at[it, at8(me), :], it)
        hub_in[it, at8(me), :] = hub_out[it, at8(me), :]

        @pl.when(it == 0)
        def _():
            for load in loads[1:]:
                load.wait()

        def tail_adj(b, cc):
            terms[pl.ds(b, 1), :] = jnp.sum(tb[b] * dbc[tail_row[b]], axis=0, keepdims=True)
            return cc

        lax.fori_loop(0, NT, tail_adj, 0, unroll=4)
        hi, mid, lo = split3(terms[...])
        tail_out[it] = mm(s3[...], jnp.concatenate([hi, mid, lo, zeros16], axis=0))
        to_rows(
            lambda p: tail_out.at[it, at8(p, CAP), :], tail_in.at[it, at8(me, CAP), :], 3 + it
        )
        tail_in[it, at8(me), :] = tail_out[it, at8(me), :]

        @pl.when(it == 0)
        def _():
            wait_bytes(slot_in.at[pl.ds(0, CAP * (ROWS - 1)), :], r_sem.at[15])
            slot_in[at8(me), :] = slot_out[at8(me), :]
            asked = jnp.where(live, slot_in[...], -1.0)
            asked_row = asked.T[0:NC, :]
            coll[...] = jnp.where(iota((NC, PL), 0).astype(F32) == asked_row, 1.0, 0.0).astype(BF16)
            lanes = iota((PL, 256), 1)
            asked2 = jnp.concatenate([asked, asked], axis=1)
            ct3[...] = jnp.where(
                (lax.rem(lanes, NC).astype(F32) == asked2) & (lanes < 3 * NC), 1.0, 0.0
            ).astype(BF16)
            wait_bytes(init_in.at[pl.ds(0, 8 * (HUBS - 1)), :], r_sem.at[16])
            init_in[at8(hub), :] = init_out[...]
            xh_state[...] = init_in[pl.ds(0, 8, stride=8), :]

        wait_bytes(hub_in.at[it, pl.ds(0, 8 * (ROWS - 1)), :], r_sem.at[it])
        part = jnp.sum(hub_in[it].reshape(ROWS, 8, BW), axis=0)
        z_out[it] = part
        to_hubs(z_out.at[it], z_in.at[it, at8(hub), :], 6 + it)
        z_in[it, at8(hub), :] = part

        wait_bytes(tail_in.at[it, pl.ds(0, CAP * (ROWS - 1)), :], r_sem.at[3 + it])
        hi, mid, lo = split3(jnp.where(live, tail_in[it], 0.0))
        cm = coll[...]
        image = mm(cm, hi) + mm(cm, mid) + mm(cm, lo)
        xt = xt_out[...]
        xn = jnp.minimum(jnp.maximum(xt - PRIMAL * (cost_tail[...] - image), 0.0), upper_tail[...])
        xt_out[...] = xn
        hi, mid, lo = split3(2.0 * xn - xt)
        ans_out[it] = mm(ct3[...], jnp.concatenate([hi, mid, lo, jnp.zeros_like(hi)], axis=0))
        to_rows(lambda p: ans_out.at[it, at8(p, CAP), :], ans_in.at[it, at8(me, CAP), :], 9 + it)
        ans_in[it, at8(me), :] = ans_out[it, at8(me), :]

        wait_bytes(z_in.at[it, pl.ds(0, 8 * (HUBS - 1)), :], r_sem.at[6 + it])
        total = jnp.sum(z_in[it].reshape(HUBS, 8, BW), axis=0)
        cost_h = init_in[pl.ds(1, 8, stride=8), :]
        upper_h = init_in[pl.ds(2, 8, stride=8), :]
        xh = xh_state[...]
        xhn = jnp.minimum(jnp.maximum(xh - PRIMAL * (cost_h - total), 0.0), upper_h)
        xh_state[...] = xhn
        extra = 2.0 * xhn - xh
        ag_out[it] = extra
        to_rows(lambda p: ag_out.at[it], ag_in.at[it, at8(me), :], 12 + it)
        ag_in[it, at8(me), :] = extra

        @pl.when(it == ITERS - 1)
        def _():
            xf_out[0] = xh_state[pl.ds(hub, 1), :]
            to_rows(lambda p: xf_out.at[0], xf_in.at[me], 17)
            xf_in[me] = xf_out[0]

        wait_bytes(ans_in.at[it, pl.ds(0, CAP * (ROWS - 1)), :], r_sem.at[9 + it])
        hi, mid, lo = split3(jnp.where(live, ans_in[it], 0.0))
        sm = st[...]
        picked[...] = mm(sm, hi) + mm(sm, mid) + mm(sm, lo)

        def tail_fwd(b, yy):
            prod = jnp.sum(tb[b] * picked[pl.ds(b, 1), :], axis=1, keepdims=True)
            return jnp.where(lane == b, prod, yy)

        yy = lax.fori_loop(0, NT, tail_fwd, jnp.zeros((BW, BW), F32), unroll=4)

        wait_bytes(ag_in.at[it, pl.ds(0, 8 * (ROWS - 1)), :], r_sem.at[12 + it])

        def hub_fwd(k, yy):
            col = hub_col[k]
            pos = lax.rem(col, ROWS) * 8 + col // ROWS
            prod = jnp.sum(hb[k] * ag_in[it, pl.ds(pos, 1), :], axis=1, keepdims=True)
            return jnp.where(lane == NT + k, prod, yy)

        yy = lax.fori_loop(0, NH, hub_fwd, yy, unroll=4)
        hi, mid, lo = split3(yy)
        rm = rp[...]
        primal = mm(hi, rm) + mm(mid, rm) + mm(lo, rm)
        d_new = jnp.maximum(d_state[...] + DUAL * (dem_t[...] - primal), 0.0)
        d_state[...] = d_new

        @pl.when(it < ITERS - 1)
        def _():
            for r in range(NR):
                dbc[r] = jnp.broadcast_to(d_new[:, r : r + 1], (BW, BW))

        return carry

    lax.fori_loop(0, ITERS, iteration, 0)

    d_out[...] = d_state[...].T[0:NR, :]
    wait_bytes(xf_in.at[pl.ds(0, ROWS - 1)], r_sem.at[17])
    for p in range(ROWS):
        xh_out[p : p + 1, :] = xf_in[p]

    full = hub_in.at[0, pl.ds(0, 8 * (ROWS - 1)), :]
    six = tail_in.at[0, pl.ds(0, CAP * (ROWS - 1)), :]
    seven = z_in.at[0, pl.ds(0, 8 * (HUBS - 1)), :]
    for it in range(ITERS):
        wait_bytes(full, s_sem.at[it])
        wait_bytes(six, s_sem.at[3 + it])
        wait_bytes(seven, s_sem.at[6 + it])
        wait_bytes(six, s_sem.at[9 + it])
        wait_bytes(full, s_sem.at[12 + it])
    wait_bytes(six, s_sem.at[15])
    wait_bytes(seven, s_sem.at[16])
    wait_bytes(xf_in.at[pl.ds(0, ROWS - 1)], s_sem.at[17])


def on_device(*args):
    vm = pl.BlockSpec(memory_space=pltpu.VMEM)
    sm = pl.BlockSpec(memory_space=pltpu.SMEM)
    hbm = pl.BlockSpec(memory_space=pltpu.HBM)
    v = lambda *s: pltpu.VMEM(s, F32)
    vb = lambda *s: pltpu.VMEM(s, BF16)
    return pl.pallas_call(
        kernel,
        out_shape=(
            jax.ShapeDtypeStruct((NC, BW), F32),
            jax.ShapeDtypeStruct((ROWS, BW), F32),
            jax.ShapeDtypeStruct((NR, BW), F32),
        ),
        in_specs=[hbm, sm, vm, sm, hbm, sm, sm] + [vm] * 8,
        out_specs=(vm, vm, vm),
        scratch_shapes=[
            v(NT, BW, BW), v(NH, BW, BW), v(NR, BW, BW),
            v(3, PL, BW), v(3, PL, BW), v(3, 8, BW), v(3, 64, BW), v(3, 8, BW), v(3, PL, BW),
            v(3, PL, BW), v(3, PL, BW), v(3, PL, BW), v(3, PL, BW),
            v(PL, BW), v(PL, BW), v(8, BW), v(64, BW), v(1, 1, BW), v(ROWS, 1, BW),
            v(TP, BW), v(HP, BW), v(TP, BW), v(BW, BW),
            vb(PL, 256), vb(PL, BW), vb(PL, 256), vb(NC, PL), vb(TP, PL), vb(BW, BW),
            v(8, BW), v(BW, BW), v(BW, BW),
            pltpu.SemaphoreType.DMA((5,)),
            pltpu.SemaphoreType.DMA((18,)),
            pltpu.SemaphoreType.DMA((18,)),
        ],
        compiler_params=pltpu.CompilerParams(
            collective_id=0, has_side_effects=True, vmem_limit_bytes=48 * 1024 * 1024
        ),
        name="pdhg",
    )(*args)


def solution(mesh):
    split = P(("rows", "hub"))
    split2 = P(("rows", "hub"), None)
    split3d = P(("rows", "hub"), None, None)
    hubs = P("hub", None)
    in_specs = (
        split3d, split, split2, split, split3d, split, split,
        split2, split2, split2, hubs, hubs, hubs, split2, split2,
    )
    return jax.shard_map(
        on_device, mesh=mesh, in_specs=in_specs, out_specs=(split2, hubs, split2), check_vma=False
    )
```

```python
import jax
import jax.numpy as jnp
from jax import lax
from jax.experimental import pallas as pl
from jax.experimental.pallas import tpu as pltpu
from jax.sharding import PartitionSpec as P

ITERS = 3
PRIMAL = 0.25
DUAL = 0.25
MESH = pl.DeviceIdType.MESH
F32 = jnp.float32
BF16 = jnp.bfloat16

NT = 72
NH = 24
NR = 16
NC = 64
CAP = 6
BW = 128
ROWS = 32
HUBS = 8
CHUNKS = 12
TP = 80
HP = 32
PL = 8 * ROWS


def hops(d):
    return min(d, 4 - d)


OFFSETS = sorted(
    [(dy, dx, dc) for dy in range(4) for dx in range(4) for dc in range(2) if dy or dx or dc],
    key=lambda o: (-(hops(o[0]) + hops(o[1])), -o[2], o[0], o[1]),
)
HUB_OFFSETS = [4, 3, 5, 2, 6, 1, 7]


def iota(shape, dim):
    return lax.broadcasted_iota(jnp.int32, shape, dim)


def split3(a):
    hi = a.astype(BF16)
    rest = a - hi.astype(F32)
    mid = rest.astype(BF16)
    lo = (rest - mid.astype(F32)).astype(BF16)
    return hi, mid, lo


def mm(a, b):
    return jnp.dot(a, b, preferred_element_type=F32)


class Scope:
    def __init__(self):
        self.now = None

    def leave(self):
        if self.now is not None:
            self.now.__exit__(None, None, None)
        self.now = None

    def enter(self, name):
        self.leave()
        self.now = jax.named_scope(name)
        self.now.__enter__()


def kernel(
    tail_hbm, tail_row_hbm, owner_hbm, tail_slot_hbm, hub_hbm, hub_row_hbm, hub_col_hbm,
    x_tail_hbm, cost_tail_hbm, upper_tail_hbm, x_hub_hbm, cost_hub_hbm, upper_hub_hbm,
    duals_hbm, demand_hbm,
    xt_out, xh_out, d_out,
    tail_row, owner, tail_slot, hub_row, hub_col,
    cost_tail, upper_tail, x_hub, cost_hub, upper_hub, duals, demand,
    tb, hb, dbc,
    hub_out, hub_in, z_out, z_in, ag_out, ag_in,
    tail_out, tail_in, ans_out, ans_in,
    slot_out, slot_in, init_out, init_in, xf_out, xf_in,
    terms, hterms, picked, colbuf, idx_v, idx, tacc, hacc, dem,
    s3, hp3, ct3, coll, st, xh_state,
    load_sem, s_sem, r_sem,
):
    me = lax.axis_index("rows")
    hub = lax.axis_index("hub")
    y, x, c = me // 8, lax.rem(me // 2, 4), lax.rem(me, 2)
    peers = [
        lax.rem(y + dy, 4) * 8 + lax.rem(x + dx, 4) * 2 + lax.rem(c + dc, 2) for dy, dx, dc in OFFSETS
    ]
    hub_peers = [lax.rem(hub + d, HUBS) for d in HUB_OFFSETS]

    def at8(i, n=8):
        return pl.ds(pl.multiple_of(i * 8, 8), n)

    pairs = [
        (owner_hbm, owner), (tail_slot_hbm, tail_slot), (hub_col_hbm, hub_col),
        (tail_row_hbm, tail_row), (hub_row_hbm, hub_row),
        (x_hub_hbm, x_hub), (cost_hub_hbm, cost_hub), (upper_hub_hbm, upper_hub),
        (duals_hbm, duals), (demand_hbm, demand), (hub_hbm, hb),
        (x_tail_hbm, xt_out), (cost_tail_hbm, cost_tail), (upper_tail_hbm, upper_tail),
    ]
    step = NT // CHUNKS
    pairs += [
        (tail_hbm.at[pl.ds(i * step, step)], tb.at[pl.ds(i * step, step)]) for i in range(CHUNKS)
    ]
    scope = Scope()
    scope.enter("start")
    loads = [pltpu.make_async_copy(s, d, load_sem.at[i]) for i, (s, d) in enumerate(pairs)]
    for load in loads:
        load.start()

    barrier = pltpu.get_barrier_semaphore()
    for p in peers:
        pl.semaphore_signal(barrier, inc=1, device_id={"rows": p}, device_id_type=MESH)
    for p in hub_peers:
        pl.semaphore_signal(barrier, inc=1, device_id={"hub": p}, device_id_type=MESH)

    def to_rows(src, dst, k):
        for p in peers:
            pltpu.make_async_remote_copy(
                src_ref=src(p), dst_ref=dst, send_sem=s_sem.at[k], recv_sem=r_sem.at[k],
                device_id={"rows": p}, device_id_type=MESH,
            ).start()

    def to_hubs(src, dst, k):
        for p in hub_peers:
            pltpu.make_async_remote_copy(
                src_ref=src, dst_ref=dst, send_sem=s_sem.at[k], recv_sem=r_sem.at[k],
                device_id={"hub": p}, device_id_type=MESH,
            ).start()

    def wait_bytes(ref, sem):
        pltpu.make_async_copy(ref, ref, sem).wait()

    loads[0].wait()
    loads[1].wait()
    for b in range(NT):
        colbuf[pl.ds(b, 1), :] = jnp.full((1, BW), tail_slot[b], jnp.int32).astype(F32)
    slot_col = jnp.where(iota((TP, BW), 0) < NT, colbuf[0:TP, :], 0.0)
    for b in range(NT):
        colbuf[pl.ds(b, 1), :] = jnp.full((1, BW), owner[b], jnp.int32).astype(F32)
    own_col = jnp.where(iota((BW, BW), 0) < NT, colbuf[...], -1.0)
    own_row = own_col.T
    sub, lane = iota((BW, BW), 0), iota((BW, BW), 1)
    before = jnp.where((own_col == own_row) & (lane < sub), 1.0, 0.0)
    within = jnp.sum(before, axis=1, keepdims=True)
    place = jnp.where(sub < NT, own_col * 8.0 + within, -1.0)
    place = place[0:TP, :]
    place3 = jnp.concatenate([place, place, place, jnp.full((16, BW), -1.0, F32)], axis=0)
    place_row = place3.T[0:1, :]
    s3[...] = jnp.where(iota((PL, 256), 0).astype(F32) == place_row, 1.0, 0.0).astype(BF16)
    st[...] = jnp.where(
        iota((TP, PL), 1).astype(F32) == jnp.concatenate([place, place], axis=1), 1.0, 0.0
    ).astype(BF16)
    zeros16 = jnp.zeros((16, BW), BF16)
    slot_b = slot_col.astype(BF16)
    zeros_tp = jnp.zeros((TP, BW), BF16)
    slot_out[...] = mm(s3[...], jnp.concatenate([slot_b, zeros_tp, zeros_tp, zeros16], axis=0))

    for load in loads[5:8]:
        load.wait()
    init_out[...] = jnp.zeros((8, BW), F32)
    init_out[0:1, :] = x_hub[pl.ds(me, 1), :]
    init_out[1:2, :] = cost_hub[pl.ds(me, 1), :]
    init_out[2:3, :] = upper_hub[pl.ds(me, 1), :]

    for load in loads[2:5]:
        load.wait()
    pos_row = jnp.full((1, BW), -1, jnp.int32)
    lane1 = iota((1, BW), 1)
    for k in range(NH):
        col = hub_col[k]
        pos = lax.rem(col, ROWS) * 8 + col // ROWS
        pos_row = jnp.where((lane1 % HP == k) & (lane1 < 3 * HP), pos, pos_row)
    hp3[...] = jnp.where(iota((PL, BW), 0) == pos_row, 1.0, 0.0).astype(BF16)

    subf, lanef = sub.astype(F32), lane.astype(F32)

    def by_row(count, at, values):
        held = jnp.where(sub < count, colbuf[...], 1000.0)
        other = held.T
        rank = jnp.sum(
            jnp.where((other < held) | ((other == held) & (lane < sub)), 1.0, 0.0),
            axis=1, keepdims=True,
        )
        here = rank == lanef

        def listed(v):
            return jnp.sum(jnp.where(here, v, 0.0), axis=0, keepdims=True)

        rows = listed(held)
        last = jnp.sum(jnp.where(held <= lanef, 1.0, 0.0), axis=0, keepdims=True)
        some = jnp.sum(jnp.where(held == lanef, 1.0, 0.0), axis=0, keepdims=True)
        keep = (rows == pltpu.roll(rows, 1, 1)) & (lane1 > 0)
        lists = [
            listed(subf),
            jnp.where(keep, 1.0, 0.0),
            jnp.where(some > 0.0, last - 1.0, 1.0 * count),
        ] + [listed(v) for v in values]
        for i, v in enumerate(lists):
            idx_v[at + i : at + i + 1, :] = v.astype(jnp.int32)

    for b in range(NT):
        colbuf[pl.ds(b, 1), :] = jnp.full((1, BW), tail_row[b], jnp.int32).astype(F32)
    by_row(NT, 0, [])
    for k in range(NH):
        col = hub_col[k]
        pos = lax.rem(col, ROWS) * 8 + col // ROWS
        colbuf[pl.ds(k, 1), :] = jnp.full((1, BW), pos, jnp.int32).astype(F32)
    pos_col = jnp.where(sub < NH, colbuf[...], 0.0)
    for k in range(NH):
        colbuf[pl.ds(k, 1), :] = jnp.full((1, BW), hub_row[k], jnp.int32).astype(F32)
    by_row(NH, 3, [pos_col])
    idx_v[7:8, :] = jnp.zeros((1, BW), jnp.int32)
    to_scalars = pltpu.make_async_copy(idx_v, idx, load_sem.at[14 + CHUNKS])
    to_scalars.start()
    tacc[NT] = jnp.zeros((BW, BW), F32)
    hacc[NH] = jnp.zeros((BW, BW), F32)

    loads[8].wait()
    loads[9].wait()
    pad = jnp.zeros((BW - NR, BW), F32)
    d_t = jnp.concatenate([duals[...], pad], axis=0).T
    dem_t = jnp.concatenate([demand[...], pad], axis=0).T
    for r in range(NR):
        dbc[r] = jnp.broadcast_to(d_t[:, r : r + 1], (BW, BW))
    for r in range(NR):
        dem[r] = jnp.broadcast_to(dem_t[:, r : r + 1], (BW, BW))

    terms[...] = jnp.zeros_like(terms)
    hterms[...] = jnp.zeros_like(hterms)
    live = lax.rem(iota((PL, BW), 0), 8) < CAP

    def listed_at(i, k, top):
        return jnp.minimum(jnp.maximum(idx[i, k], 0), top)

    def hub_adjoint(it):
        for k in range(NH):
            hterms[k : k + 1, :] = jnp.sum(hb[k] * dbc[hub_row[k]], axis=0, keepdims=True)
        hi, mid, lo = split3(hterms[...])
        hub_out[it] = mm(hp3[...], jnp.concatenate([hi, mid, lo, jnp.zeros_like(hi)], axis=0))

    scope.enter("wait_hb")
    loads[10].wait()
    scope.enter("adj_hub0")
    hub_adjoint(0)
    to_scalars.wait()

    scope.enter("wait_barrier")
    pl.semaphore_wait(barrier, len(OFFSETS) + len(HUB_OFFSETS))
    scope.leave()

    def iteration(it, carry):
        scope.enter("rs_send")
        to_rows(lambda p: hub_out.at[it, at8(p), :], hub_in.at[it, at8(me), :], it)
        hub_in[it, at8(me), :] = hub_out[it, at8(me), :]

        @pl.when(it == 0)
        def _():
            to_hubs(init_out, init_in.at[at8(hub), :], 16)
            to_rows(lambda p: slot_out.at[at8(p, CAP), :], slot_in.at[at8(me, CAP), :], 15)

        scope.enter("adj_tail")
        @pl.when(it == 0)
        def _():
            for load in loads[11:]:
                load.wait()

        def tail_adj(b, cc):
            terms[pl.ds(b, 1), :] = jnp.sum(tb[b] * dbc[tail_row[b]], axis=0, keepdims=True)
            return cc

        lax.fori_loop(0, NT, tail_adj, 0, unroll=4)
        hi, mid, lo = split3(terms[...])
        tail_out[it] = mm(s3[...], jnp.concatenate([hi, mid, lo, zeros16], axis=0))
        to_rows(
            lambda p: tail_out.at[it, at8(p, CAP), :], tail_in.at[it, at8(me, CAP), :], 3 + it
        )
        tail_in[it, at8(me), :] = tail_out[it, at8(me), :]

        @pl.when(it == 0)
        def _():
            wait_bytes(slot_in.at[pl.ds(0, CAP * (ROWS - 1)), :], r_sem.at[15])
            slot_in[at8(me), :] = slot_out[at8(me), :]
            asked = jnp.where(live, slot_in[...], -1.0)
            asked_row = asked.T[0:NC, :]
            coll[...] = jnp.where(iota((NC, PL), 0).astype(F32) == asked_row, 1.0, 0.0).astype(BF16)
            lanes = iota((PL, 256), 1)
            asked2 = jnp.concatenate([asked, asked], axis=1)
            ct3[...] = jnp.where(
                (lax.rem(lanes, NC).astype(F32) == asked2) & (lanes < 3 * NC), 1.0, 0.0
            ).astype(BF16)
            wait_bytes(init_in.at[pl.ds(0, 8 * (HUBS - 1)), :], r_sem.at[16])
            init_in[at8(hub), :] = init_out[...]
            xh_state[...] = init_in[pl.ds(0, 8, stride=8), :]

        scope.enter("wait_rs")
        wait_bytes(hub_in.at[it, pl.ds(0, 8 * (ROWS - 1)), :], r_sem.at[it])
        scope.enter("z_send")
        part = jnp.sum(hub_in[it].reshape(ROWS, 8, BW), axis=0)
        z_out[it] = part
        to_hubs(z_out.at[it], z_in.at[it, at8(hub), :], 6 + it)
        z_in[it, at8(hub), :] = part

        scope.enter("wait_tail")
        wait_bytes(tail_in.at[it, pl.ds(0, CAP * (ROWS - 1)), :], r_sem.at[3 + it])
        scope.enter("tail_update")
        hi, mid, lo = split3(jnp.where(live, tail_in[it], 0.0))
        cm = coll[...]
        image = mm(cm, hi) + mm(cm, mid) + mm(cm, lo)
        xt = xt_out[...]
        xn = jnp.minimum(jnp.maximum(xt - PRIMAL * (cost_tail[...] - image), 0.0), upper_tail[...])
        xt_out[...] = xn
        hi, mid, lo = split3(2.0 * xn - xt)
        ans_out[it] = mm(ct3[...], jnp.concatenate([hi, mid, lo, jnp.zeros_like(hi)], axis=0))
        to_rows(lambda p: ans_out.at[it, at8(p, CAP), :], ans_in.at[it, at8(me, CAP), :], 9 + it)
        ans_in[it, at8(me), :] = ans_out[it, at8(me), :]

        scope.enter("wait_z")
        wait_bytes(z_in.at[it, pl.ds(0, 8 * (HUBS - 1)), :], r_sem.at[6 + it])
        scope.enter("hub_update")
        total = jnp.sum(z_in[it].reshape(HUBS, 8, BW), axis=0)
        cost_h = init_in[pl.ds(1, 8, stride=8), :]
        upper_h = init_in[pl.ds(2, 8, stride=8), :]
        xh = xh_state[...]
        xhn = jnp.minimum(jnp.maximum(xh - PRIMAL * (cost_h - total), 0.0), upper_h)
        xh_state[...] = xhn
        extra = 2.0 * xhn - xh
        ag_out[it] = extra
        to_rows(lambda p: ag_out.at[it], ag_in.at[it, at8(me), :], 12 + it)
        ag_in[it, at8(me), :] = extra

        @pl.when(it == ITERS - 1)
        def _():
            xf_out[0] = xh_state[pl.ds(hub, 1), :]
            to_rows(lambda p: xf_out.at[0], xf_in.at[me], 17)
            xf_in[me] = xf_out[0]

        scope.enter("wait_ans")
        wait_bytes(ans_in.at[it, pl.ds(0, CAP * (ROWS - 1)), :], r_sem.at[9 + it])
        scope.enter("fwd_tail")
        hi, mid, lo = split3(jnp.where(live, ans_in[it], 0.0))
        sm = st[...]
        picked[...] = mm(sm, hi) + mm(sm, mid) + mm(sm, lo)

        def tail_fwd(k, acc):
            i = listed_at(0, k, NT - 1)
            acc = acc * idx[1, k].astype(F32) + tb[i] * picked[pl.ds(i, 1), :]
            tacc[k] = acc
            return acc

        lax.fori_loop(0, NT, tail_fwd, jnp.zeros((BW, BW), F32), unroll=8)

        scope.enter("wait_ag")
        wait_bytes(ag_in.at[it, pl.ds(0, 8 * (ROWS - 1)), :], r_sem.at[12 + it])

        scope.enter("fwd_hub")
        acc = jnp.zeros((BW, BW), F32)
        for k in range(NH):
            acc = acc * idx[4, k].astype(F32) + hb[listed_at(3, k, NH - 1)] * ag_in[it, pl.ds(listed_at(6, k, PL - 1), 1), :]
            hacc[k] = acc
        scope.enter("dual")
        for r in range(NR):
            image = jnp.sum(
                tacc[listed_at(2, r, NT)] + hacc[listed_at(5, r, NH)], axis=1, keepdims=True
            )
            dbc[r] = jnp.maximum(dbc[r] + DUAL * (dem[r] - image), 0.0)

        @pl.when(it < ITERS - 1)
        def _():
            with jax.named_scope("adj_hub"):
                hub_adjoint(it + 1)

        scope.leave()
        return carry

    lax.fori_loop(0, ITERS, iteration, 0)

    scope.enter("finish")
    narrow = jnp.zeros((BW, BW), F32)
    for r in range(NR):
        narrow = jnp.where(lane == r, dbc[r], narrow)
    d_out[...] = narrow.T[0:NR, :]
    wait_bytes(xf_in.at[pl.ds(0, ROWS - 1)], r_sem.at[17])
    for p in range(ROWS):
        xh_out[p : p + 1, :] = xf_in[p]

    full = hub_in.at[0, pl.ds(0, 8 * (ROWS - 1)), :]
    six = tail_in.at[0, pl.ds(0, CAP * (ROWS - 1)), :]
    seven = z_in.at[0, pl.ds(0, 8 * (HUBS - 1)), :]
    for it in range(ITERS):
        wait_bytes(full, s_sem.at[it])
        wait_bytes(six, s_sem.at[3 + it])
        wait_bytes(seven, s_sem.at[6 + it])
        wait_bytes(six, s_sem.at[9 + it])
        wait_bytes(full, s_sem.at[12 + it])
    wait_bytes(six, s_sem.at[15])
    wait_bytes(seven, s_sem.at[16])
    wait_bytes(xf_in.at[pl.ds(0, ROWS - 1)], s_sem.at[17])
    scope.leave()


def writer(a_ref, b_ref, c_ref, a_out, b_out, c_out, sem):
    copies = [
        pltpu.make_async_copy(src, dst, sem.at[i])
        for i, (src, dst) in enumerate([(a_ref, a_out), (b_ref, b_out), (c_ref, c_out)])
    ]
    for copy in copies:
        copy.start()
    for copy in copies:
        copy.wait()


def on_device(*args):
    args = list(args)
    args[2] = args[2].reshape(NT)
    vm = pl.BlockSpec(memory_space=pltpu.VMEM)
    hbm = pl.BlockSpec(memory_space=pltpu.HBM)
    args = [pltpu.with_memory_space_constraint(a, pltpu.HBM) for a in args]
    v = lambda *s: pltpu.VMEM(s, F32)
    si = lambda n: pltpu.SMEM((n,), jnp.int32)
    vb = lambda *s: pltpu.VMEM(s, BF16)
    outs = [(NC, BW), (ROWS, BW), (NR, BW)]
    held = pl.pallas_call(
        kernel,
        out_shape=tuple(pltpu.VMEM(s, F32) for s in outs),
        in_specs=[hbm] * 15,
        out_specs=(vm, vm, vm),
        scratch_shapes=[
            si(NT), si(NT), si(NT), si(NH), si(NH),
            v(NC, BW), v(NC, BW), v(ROWS, BW), v(ROWS, BW), v(ROWS, BW), v(NR, BW), v(NR, BW),
            v(NT, BW, BW), v(NH, BW, BW), v(NR, BW, BW),
            v(3, PL, BW), v(3, PL, BW), v(3, 8, BW), v(3, 64, BW), v(3, 8, BW), v(3, PL, BW),
            v(3, PL, BW), v(3, PL, BW), v(3, PL, BW), v(3, PL, BW),
            v(PL, BW), v(PL, BW), v(8, BW), v(64, BW), v(1, 1, BW), v(ROWS, 1, BW),
            v(TP, BW), v(HP, BW), v(TP, BW), v(BW, BW),
            pltpu.VMEM((8, BW), jnp.int32), pltpu.SMEM((8, BW), jnp.int32),
            v(NT + 1, BW, BW), v(NH + 1, BW, BW), v(NR, BW, BW),
            vb(PL, 256), vb(PL, BW), vb(PL, 256), vb(NC, PL), vb(TP, PL), v(8, BW),
            pltpu.SemaphoreType.DMA((15 + CHUNKS,)),
            pltpu.SemaphoreType.DMA((18,)),
            pltpu.SemaphoreType.DMA((18,)),
        ],
        compiler_params=pltpu.CompilerParams(
            collective_id=0, has_side_effects=True, vmem_limit_bytes=32 * 1024 * 1024
        ),
        name="pdhg",
    )(*args)
    return pl.pallas_call(
        writer,
        out_shape=tuple(jax.ShapeDtypeStruct(s, F32) for s in outs),
        in_specs=[vm, vm, vm],
        out_specs=(hbm, hbm, hbm),
        scratch_shapes=[pltpu.SemaphoreType.DMA((3,))],
        compiler_params=pltpu.CompilerParams(vmem_limit_bytes=1024 * 1024),
        name="writer",
    )(*held)


def solution(mesh):
    split = P(("rows", "hub"))
    split2 = P(("rows", "hub"), None)
    split3d = P(("rows", "hub"), None, None)
    hubs = P("hub", None)
    in_specs = (
        split3d, split, split2, split, split3d, split, split,
        split2, split2, split2, hubs, hubs, hubs, split2, split2,
    )
    return jax.shard_map(
        on_device, mesh=mesh, in_specs=in_specs, out_specs=(split2, hubs, split2), check_vma=False
    )
```
